8 devices in a mesh: data: 8 (over z, y, x, core).
Axes of the slice: x: 2, y: 2, z: 1, core: 2. Of those that a mesh axis runs over, the one named last changes fastest.
Arguments:
- acts_in: bfloat16 [16, 3, 512, 1536], P('data')
- grad_out: bfloat16 [16, 3, 512, 1536], P('data')
- w_up: bfloat16 [3, 1536, 6144], replicated
- w_down: bfloat16 [3, 6144, 1536], replicated
- clip_norm: float32 [1], replicated
Outputs:
- output 1: bfloat16 [3, 1536, 6144], replicated
- output 2: bfloat16 [3, 6144, 1536], replicated
- output 3: bfloat16 [16, 3, 512, 1536], P('data')
All inputs are finite; a program needn't handle non-finite values.
Results may differ from the reference program's by a relative error of at most 0.0145307.
Values are sent between devices in bfloat16 or wider.
A program may use at most 1 GiB of HBM per device.

```python
import math
import jax
import jax.numpy as jnp
from jax import lax

NUM_DEVICES = 8
MICROBATCHES = 2
MICRO_SEQS = 3
SEQ_LEN = 512
MODEL_DIM = 1536
LAYERS = 3
HIDDEN_DIM = 4 * MODEL_DIM


def gelu_tanh(values):
    return jax.nn.gelu(values, approximate=True)


def setup_inputs(seed: int = 0) -> dict:
    key_list = jax.random.split(jax.random.key(seed), 5)
    block_shape = (NUM_DEVICES * MICROBATCHES, MICRO_SEQS, SEQ_LEN, MODEL_DIM)
    acts_in = jax.random.normal(key_list[0], block_shape, jnp.float32).astype(jnp.bfloat16)
    grad_out = jax.random.normal(key_list[1], block_shape, jnp.float32).astype(jnp.bfloat16)
    w_up = (jax.random.normal(key_list[2], (LAYERS, MODEL_DIM, HIDDEN_DIM), jnp.float32) * MODEL_DIM ** -0.5).astype(jnp.bfloat16)
    w_down = (jax.random.normal(key_list[3], (LAYERS, HIDDEN_DIM, MODEL_DIM), jnp.float32) * HIDDEN_DIM ** -0.5).astype(jnp.bfloat16)
    clip_norm = jax.random.uniform(key_list[4], (1,), jnp.float32, 0.5, 1.0) * (math.sqrt(8 * LAYERS) * MODEL_DIM)
    return {'acts_in': acts_in, 'grad_out': grad_out, 'w_up': w_up, 'w_down': w_down, 'clip_norm': clip_norm}


def micro_step(x_rows, dy_rows, w_up, w_down):
    saved_acts = []
    hidden = x_rows
    for layer_idx in range(LAYERS):
        pre_act = jnp.dot(hidden, w_up[layer_idx], preferred_element_type=jnp.float32).astype(jnp.bfloat16)
        gelu_out = gelu_tanh(pre_act.astype(jnp.float32)).astype(jnp.bfloat16)
        saved_acts.append((hidden, pre_act, gelu_out))
        hidden = (hidden.astype(jnp.float32) + jnp.dot(gelu_out, w_down[layer_idx], preferred_element_type=jnp.float32)).astype(jnp.bfloat16)
    back_grad = dy_rows
    up_list = [None] * LAYERS
    down_list = [None] * LAYERS
    for layer_idx in range(LAYERS - 1, -1, -1):
        hidden, pre_act, gelu_out = saved_acts[layer_idx]
        down_list[layer_idx] = jnp.dot(gelu_out.T, back_grad, preferred_element_type=jnp.float32)
        act_grad = jnp.dot(back_grad, w_down[layer_idx].T, preferred_element_type=jnp.float32)
        gelu_back = jax.vjp(gelu_tanh, pre_act.astype(jnp.float32))[1]
        pre_grad = gelu_back(act_grad)[0].astype(jnp.bfloat16)
        up_list[layer_idx] = jnp.dot(hidden.T, pre_grad, preferred_element_type=jnp.float32)
        back_grad = (back_grad.astype(jnp.float32) + jnp.dot(pre_grad, w_up[layer_idx].T, preferred_element_type=jnp.float32)).astype(jnp.bfloat16)
    return jnp.stack(up_list), jnp.stack(down_list), back_grad


def reference(acts_in, grad_out, w_up, w_down, clip_norm):
    micro_count = NUM_DEVICES * MICROBATCHES
    tok_rows = MICRO_SEQS * SEQ_LEN
    x_micro = acts_in.reshape(micro_count, tok_rows, MODEL_DIM)
    dy_micro = grad_out.reshape(micro_count, tok_rows, MODEL_DIM)

    def step_fn(carry_in, mb_pair):
        up_acc, down_acc = carry_in
        up_step, down_step, dx_rows = micro_step(mb_pair[0], mb_pair[1], w_up, w_down)
        return (up_acc + up_step, down_acc + down_step), dx_rows

    init_acc = (jnp.zeros((LAYERS, MODEL_DIM, HIDDEN_DIM), jnp.float32), jnp.zeros((LAYERS, HIDDEN_DIM, MODEL_DIM), jnp.float32))
    acc_sums, dx_micro = lax.scan(step_fn, init_acc, (x_micro, dy_micro))
    up_sum, down_sum = acc_sums
    total_norm = jnp.sqrt(jnp.sum(up_sum * up_sum) + jnp.sum(down_sum * down_sum))
    clip_scale = jnp.minimum(1.0, clip_norm[0] / total_norm)
    grad_up = (up_sum * clip_scale).astype(jnp.bfloat16)
    grad_down = (down_sum * clip_scale).astype(jnp.bfloat16)
    return grad_up, grad_down, dx_micro.reshape(acts_in.shape)
```

```python
import jax
import jax.numpy as jnp
from jax import lax
from jax.sharding import PartitionSpec as P

FIRST_SPLIT = 2


def gelu_tanh(values):
    return jax.nn.gelu(values, approximate=True)


def matmul(lhs, rhs):
    return jnp.dot(lhs, rhs, preferred_element_type=jnp.float32)


def matmul_tokens(lhs, rhs):
    return lax.dot_general(lhs, rhs, (((0,), (0,)), ((), ())), preferred_element_type=jnp.float32)


def matmul_right(lhs, rhs):
    return lax.dot_general(lhs, rhs, (((1,), (1,)), ((), ())), preferred_element_type=jnp.float32)


def scatter_sum(grad):
    return lax.psum_scatter(grad.astype(jnp.bfloat16), 'data', scatter_dimension=0, tiled=True)


def gather(part):
    return lax.all_gather(part, 'data', axis=0, tiled=True)


def solution(mesh):
    def device_step(acts_in, grad_out, w_up, w_down, clip_norm):
        layer_count, model_width, hidden_width = w_up.shape
        hidden = acts_in.reshape(-1, model_width)
        back_grad = grad_out.reshape(-1, model_width)
        saved_acts = []
        for layer in range(layer_count):
            pre_act = matmul(hidden, w_up[layer]).astype(jnp.bfloat16)
            gelu_out = gelu_tanh(pre_act.astype(jnp.float32)).astype(jnp.bfloat16)
            saved_acts.append((hidden, pre_act, gelu_out))
            if layer < layer_count - 1:
                hidden = (hidden.astype(jnp.float32) + matmul(gelu_out, w_down[layer])).astype(jnp.bfloat16)

        squares = []

        def settle(value, stage_list):
            flat, tree = jax.tree.flatten((value, stage_list))
            return jax.tree.unflatten(tree, lax.optimization_barrier(flat))

        reduced = []
        gathering = []
        settled = {}

        def advance(value, count):
            nonlocal reduced, gathering
            ready, reduced = reduced[:count], reduced[count:]
            value, (parts, full) = settle(value, ([p for _, p in ready], [g for _, g in gathering]))
            settled.update({name: g for (name, _), g in zip(gathering, full)})
            gathering = []
            for (name, _), part in zip(ready, parts):
                squares.append(sum(jnp.sum(jnp.square(p.astype(jnp.float32))) for p in part))
                gathering.append((name, [gather(p) for p in part]))
            return value

        last = layer_count - 1
        for layer in range(last, -1, -1):
            hidden, pre_act, gelu_out = saved_acts[layer]
            pieces = FIRST_SPLIT if layer == last else 1
            width = hidden_width // pieces
            reduced.append((
                ('down', layer),
                [scatter_sum(matmul_tokens(gelu_out[:, i * width:(i + 1) * width], back_grad)) for i in range(pieces)],
            ))
            act_grad = matmul_right(back_grad, w_down[layer])
            gelu_back = jax.vjp(gelu_tanh, pre_act.astype(jnp.float32))[1]
            pre_grad = gelu_back(act_grad)[0].astype(jnp.bfloat16)
            pre_grad = advance(pre_grad, 1)
            if layer == 0:
                zero, pre_grad = settle(jnp.zeros((), jnp.bfloat16), pre_grad)
                buffers = (jnp.broadcast_to(zero, w_up.shape), jnp.broadcast_to(zero, w_down.shape))
                pre_grad, buffers = settle(pre_grad, buffers)
            reduced.append((('up', layer), [scatter_sum(matmul_tokens(hidden, pre_grad))]))
            back_grad = (back_grad.astype(jnp.float32) + matmul_right(pre_grad, w_up[layer])).astype(jnp.bfloat16)
            if 0 < layer < last:
                back_grad = advance(back_grad, 1)

        for name, part in reduced:
            squares.append(sum(jnp.sum(jnp.square(p.astype(jnp.float32))) for p in part))
            gathering.append((name, [gather(p) for p in part]))
        settled.update(gathering)
        sq_total = lax.psum(sum(squares), 'data')
        clip_scale = jnp.minimum(1.0, clip_norm[0] * lax.rsqrt(sq_total))

        def scaled(values):
            return (values.astype(jnp.float32) * clip_scale).astype(jnp.bfloat16)

        grads = {'up': buffers[0], 'down': buffers[1]}
        for (kind, layer), pieces in settled.items():
            row = 0
            for piece in pieces:
                grads[kind] = lax.dynamic_update_slice(grads[kind], scaled(piece)[None], (layer, row, 0))
                row += piece.shape[0]
        return grads['up'], grads['down'], back_grad.reshape(acts_in.shape)

    return jax.shard_map(
        device_step,
        mesh=mesh,
        in_specs=(P('data'), P('data'), P(), P(), P()),
        out_specs=(P(), P(), P('data')),
        check_vma=False,
    )
```
